8 devices in a mesh: fsdp: 8 (over z, y, x, core).
Axes of the slice: x: 2, y: 2, z: 1, core: 2. Of those that a mesh axis runs over, the one named last changes fastest.
Arguments:
- x: bfloat16 [4, 32768, 768], P(None, 'fsdp')
- g: bfloat16 [4, 32768, 768], P(None, 'fsdp')
- w1: bfloat16 [2, 768, 3072], P(None, 'fsdp')
- w2: bfloat16 [2, 3072, 768], P(None, 'fsdp')
Outputs:
- output 1: bfloat16 [4, 32768, 768], P(None, 'fsdp')
- output 2: float32 [2, 768, 3072], P(None, 'fsdp')
- output 3: float32 [2, 3072, 768], P(None, 'fsdp')
All inputs are finite; a program needn't handle non-finite values.
Results may differ from the reference program's by a relative error of at most 0.011625.
Values are sent between devices in bfloat16 or wider.
A program may use at most 1 GiB of HBM per device.

```python
import jax
import jax.numpy as jnp
from jax import lax

D = 768
FF = 3072
LAYERS = 2
MICRO = 4
TOKENS = 32768


def setup_inputs(seed: int = 0) -> dict:
    k1, k2, k3, k4 = jax.random.split(jax.random.key(seed), 4)
    w1 = jax.random.normal(k1, (LAYERS, D, FF), jnp.float32) * D ** -0.5
    w2 = jax.random.normal(k2, (LAYERS, FF, D), jnp.float32) * FF ** -0.5
    x = jax.random.normal(k3, (MICRO, TOKENS, D), jnp.float32)
    g = jax.random.normal(k4, (MICRO, TOKENS, D), jnp.float32) * (MICRO * TOKENS) ** -0.5
    return {"x": x.astype(jnp.bfloat16), "g": g.astype(jnp.bfloat16),
            "w1": w1.astype(jnp.bfloat16), "w2": w2.astype(jnp.bfloat16)}


def _gelu_bwd(a, e):
    return jax.vjp(jax.nn.gelu, a)[1](e)[0]


def _micro(w1, w2, x, g):
    def fwd(xl, ws):
        v1, v2 = ws
        a = jnp.dot(xl, v1, preferred_element_type=jnp.float32).astype(jnp.bfloat16)
        h = jax.nn.gelu(a.astype(jnp.float32)).astype(jnp.bfloat16)
        y = (xl.astype(jnp.float32) + jnp.dot(h, v2, preferred_element_type=jnp.float32)).astype(jnp.bfloat16)
        return y, (xl, a)

    y, (xs, acts) = lax.scan(fwd, x, (w1, w2))

    def bwd(gy, inp):
        v1, v2, xl, a = inp
        h = jax.nn.gelu(a.astype(jnp.float32)).astype(jnp.bfloat16)
        e = jnp.dot(gy, v2.T, preferred_element_type=jnp.float32)
        da = _gelu_bwd(a.astype(jnp.float32), e).astype(jnp.bfloat16)
        dw2 = jnp.dot(h.T, gy, preferred_element_type=jnp.float32)
        dw1 = jnp.dot(xl.T, da, preferred_element_type=jnp.float32)
        gx = (gy.astype(jnp.float32) + jnp.dot(da, v1.T, preferred_element_type=jnp.float32)).astype(jnp.bfloat16)
        return gx, (dw1, dw2)

    _, (dw1, dw2) = lax.scan(bwd, g, (w1, w2, xs, acts), reverse=True)
    return y, dw1, dw2


def reference(x, g, w1, w2):
    def step(acc, xg):
        y, dw1, dw2 = _micro(w1, w2, xg[0], xg[1])
        return (acc[0] + dw1, acc[1] + dw2), y

    zeros = (jnp.zeros(w1.shape, jnp.float32), jnp.zeros(w2.shape, jnp.float32))
    (dw1, dw2), y = lax.scan(step, zeros, (x, g))
    return (y, dw1, dw2)
```

```python
import functools
import math

import jax
import jax.numpy as jnp
from jax import lax
from jax.experimental import pallas as pl
from jax.experimental.pallas import tpu as pltpu
from jax.sharding import PartitionSpec as P

AX = "fsdp"
D, FF = 768, 3072
G0 = 768
HS = 1536
C0 = math.sqrt(2 / math.pi)
C1 = C0 * 0.044715
BF, F32 = jnp.bfloat16, jnp.float32


def gelu(a):
    t = jnp.tanh(a * (C0 + C1 * (a * a)))
    return a * (0.5 + 0.5 * t)


def gelu_grad(a):
    b = a * a
    s = 0.5 + 0.5 * jnp.tanh(a * (C0 + C1 * b))
    return s + ((a * s) * (1 - s)) * (2 * C0 + 6 * C1 * b)


def dot(a, b):
    return jnp.dot(a, b, preferred_element_type=F32)


def dot_nt(a, b):
    return lax.dot_general(a, b, (((1,), (1,)), ((), ())), preferred_element_type=F32)


def h_of(a):
    return gelu(a.astype(F32)).astype(BF)


def full(shape):
    return pl.BlockSpec(shape, lambda i: (0,) * len(shape), pipeline_mode=pl.Buffered(1))


def tok(bt, n):
    return pl.BlockSpec((bt, n), lambda i: (i, 0))


def sds(shape, dt=BF):
    return jax.ShapeDtypeStruct(shape, dt)


def call(name, body, t, bt, args, in_specs, out_specs, out_shape, scratch, dots):
    nbytes = sum(math.prod(v.shape) * v.dtype.itemsize for v in (*args, *out_shape))
    return pl.pallas_call(
        body, name=name, grid=(t // bt,), in_specs=in_specs, out_specs=out_specs, out_shape=out_shape,
        scratch_shapes=scratch,
        compiler_params=pltpu.CompilerParams(dimension_semantics=("arbitrary",), vmem_limit_bytes=67043328),
        cost_estimate=pl.CostEstimate(flops=int(dots * 2 * t * D * FF), bytes_accessed=nbytes, transcendentals=t * FF),
    )(*args)


def chunks(n, ch):
    return [slice(k, k + ch) for k in range(0, n, ch)]


def fwd_a(x, w, bt=1024, ch=256, h_from=None):
    t, n = x.shape[0], w.shape[1]

    def body(x_ref, w_ref, a_ref, *h_ref):
        lo = n if h_from is None else h_from
        prev = None
        for s in chunks(n, ch)[lo // ch:] + chunks(lo, ch):
            a = dot(x_ref[...], w_ref[:, s]).astype(BF)
            a_ref[:, s] = a
            if prev is not None:
                p, v = prev
                h_ref[0][:, p.start - lo:p.stop - lo] = h_of(v)
            prev = (s, a) if s.start >= lo else None

    widths = [n] if h_from is None else [n, n - h_from]
    return call(f"fwd_a{n}", body, t, bt, (x, w), [tok(bt, D), full((D, n))],
                [tok(bt, k) for k in widths], [sds((t, k)) for k in widths], [], n / FF)


def fwd_y0(x, a0, a1, h1, w2, bt=1024, ch=256):
    t = x.shape[0]

    def body(x_ref, a0_ref, a1_ref, h1_ref, w2_ref, y_ref, h_ref):
        for s in chunks(G0, ch):
            h_ref[:, s] = h_of(a0_ref[:, s])
        for s in chunks(HS - G0, ch):
            h_ref[:, G0 + s.start:G0 + s.stop] = h_of(a1_ref[:, s])
        p = dot(h1_ref[...], w2_ref[HS:, :]) + dot(h_ref[...], w2_ref[:HS, :])
        y_ref[...] = (x_ref[...].astype(F32) + p).astype(BF)

    return call("fwd_y0", body, t, bt, (x, a0, a1, h1, w2),
                [tok(bt, D), tok(bt, G0), tok(bt, HS - G0), tok(bt, FF - HS), full((FF, D))],
                [tok(bt, D)], [sds((t, D))], [pltpu.VMEM((bt, HS), BF)], 1)[0]


def fwd_y(x, h, w2, bt=1024):
    t = x.shape[0]

    def body(x_ref, h_ref, w2_ref, y_ref):
        y_ref[...] = (x_ref[...].astype(F32) + dot(h_ref[...], w2_ref[...])).astype(BF)

    return call("fwd_y", body, t, bt, (x, h, w2), [tok(bt, D), tok(bt, FF), full((FF, D))],
                [tok(bt, D)], [sds((t, D))], [], 1)[0]


def zero_first(ref):
    @pl.when(pl.program_id(0) == 0)
    def _():
        ref[...] = jnp.zeros_like(ref)


def put_last(steps, acc, out_ref, sem):
    @pl.when(pl.program_id(0) == steps - 1)
    def _():
        n, _, w = out_ref.shape
        copies = [pltpu.make_async_copy(acc.at[:, k * w:(k + 1) * w], out_ref.at[k], sem.at[k]) for k in range(n)]
        for c in copies:
            c.start()
        for c in copies:
            c.wait()


def fwd_dw2(x, g, w1, n, bt=512, ch=512):
    t = x.shape[0]

    def body(x_ref, g_ref, w1_ref, a_ref, h_ref, out_ref, acc, gT, sem):
        zero_first(acc)
        ss = chunks(FF, ch)

        def first(s):
            a = dot(x_ref[...], w1_ref[:, s]).astype(BF)
            a_ref[:, s] = a
            return a

        a, prev = first(ss[0]), None
        gT[...] = g_ref[...].T
        for j, s in enumerate(ss):
            nxt = first(ss[j + 1]) if j + 1 < len(ss) else None
            h = h_of(a)
            h_ref[:, s] = h
            if prev is not None:
                acc[:, ss[j - 1]] += dot(gT[...], prev)
            a, prev = nxt, h
        acc[:, ss[-1]] += dot(gT[...], prev)
        put_last(t // bt, acc, out_ref, sem)

    return call("fwd_dw2", body, t, bt, (x, g, w1), [tok(bt, D), tok(bt, D), full((D, FF))],
                [tok(bt, FF), tok(bt, FF), pl.BlockSpec(memory_space=pl.ANY)],
                [sds((t, FF)), sds((t, FF)), sds((n, D, FF // n), F32)],
                [pltpu.VMEM((D, FF), F32), pltpu.VMEM((D, bt), BF), pltpu.SemaphoreType.DMA((n,))], 2)


def dw2_0(g, a0, a1, h1, n, bt=1024, ch=512):
    t = g.shape[0]

    def body(g_ref, a0_ref, a1_ref, h1_ref, out_ref, acc, gT, h_ref, sem):
        zero_first(acc)
        gT[...] = g_ref[...].T
        for s in chunks(G0, 256):
            h_ref[:, s] = h_of(a0_ref[:, s])
        for s in chunks(HS - G0, 256):
            h_ref[:, G0 + s.start:G0 + s.stop] = h_of(a1_ref[:, s])
        for s in chunks(FF - HS, ch):
            acc[:, HS + s.start:HS + s.stop] += dot(gT[...], h1_ref[:, s])
        for s in chunks(HS, ch):
            acc[:, s] += dot(gT[...], h_ref[:, s])
        put_last(t // bt, acc, out_ref, sem)

    return call("dw2_0", body, t, bt, (g, a0, a1, h1),
                [tok(bt, D), tok(bt, G0), tok(bt, HS - G0), tok(bt, FF - HS)],
                [pl.BlockSpec(memory_space=pl.ANY)], [sds((n, D, FF // n), F32)],
                [pltpu.VMEM((D, FF), F32), pltpu.VMEM((D, bt), BF), pltpu.VMEM((bt, HS), BF),
                 pltpu.SemaphoreType.DMA((n,))], 1)[0]


def bwd(x, g, a, w2, w1=None, bt=512, ch=256, gq=1536):
    t = x.shape[0]
    na = len(a)

    def body(*refs):
        x_ref, g_ref, w2_ref, *rest = refs
        a_refs, rest = rest[:na], rest[na:]
        if w1 is None:
            dw_ref, xT = rest
        else:
            w1_ref, gx_ref, dw_ref, xT, gx_acc, da_ref = rest
        zero_first(dw_ref)
        work, off = [], 0
        for r in a_refs:
            for s in chunks(r.shape[1], ch):
                work.append((slice(off + s.start, off + s.stop), r, s))
            off += r.shape[1]

        def cot(k):
            return dot_nt(g_ref[...], w2_ref[work[k][0], :])

        def use(k, da):
            s = work[k][0]
            dw_ref[:, s] += dot(xT[...], da)
            if w1 is not None and s.stop % gq == 0:
                q = slice(s.stop - gq, s.stop)
                p = dot_nt(da_ref[:, q], w1_ref[:, q])
                if q.start:
                    p += gx_acc[...]
                if q.stop < FF:
                    gx_acc[...] = p
                else:
                    gx_ref[...] = (g_ref[...].astype(F32) + p).astype(BF)

        e, prev = cot(0), None
        xT[...] = x_ref[...].T
        for k, (_, r, s) in enumerate(work):
            nxt = cot(k + 1) if k + 1 < len(work) else None
            da = (gelu_grad(r[:, s].astype(F32)) * e).astype(BF)
            if w1 is not None:
                da_ref[:, work[k][0]] = da
            if prev is not None:
                use(k - 1, prev)
            e, prev = nxt, da
        use(len(work) - 1, prev)

    args, specs = [x, g, w2, *a], [tok(bt, D), tok(bt, D), full((FF, D)), *(tok(bt, v.shape[1]) for v in a)]
    outs, oshape = [full((D, FF))], [sds((D, FF), F32)]
    scratch = [pltpu.VMEM((D, bt), BF)]
    if w1 is not None:
        args, specs = [*args, w1], [*specs, full((D, FF))]
        outs, oshape = [tok(bt, D), *outs], [sds((t, D)), *oshape]
        scratch += [pltpu.VMEM((bt, D), F32), pltpu.VMEM((bt, FF), BF)]
    return call("bwd" if w1 is not None else "bwd0", body, t, bt, tuple(args), specs, outs, oshape, scratch,
                2 if w1 is None else 3)


def solution(mesh):
    spec = P(None, AX, None)
    n = mesh.shape[AX]

    def gather(w):
        return lax.all_gather(w, AX, axis=0, tiled=True)

    def scatter(v):
        return lax.psum_scatter(v, AX, scatter_dimension=0, tiled=True)

    def after(v, *done):
        return lax.optimization_barrier((v, *done))[0]

    def body(x, g, w1, w2):
        shape = x.shape
        x, g = x.reshape(-1, D), g.reshape(-1, D)
        w10a, w10b = gather(w1[0, :, :G0]), gather(w1[0, :, G0:])
        w20, w11, w21 = gather(w2[0]), gather(w1[1]), gather(w2[1])
        a0, = fwd_a(x, w10a)
        a1, h1 = fwd_a(after(x, a0), w10b, h_from=HS - G0)
        x1 = fwd_y0(x, a0, a1, h1, w20)
        a, h, p21 = fwd_dw2(x1, g, w11, n)
        s21 = scatter(p21)
        gx, p11 = bwd(x1, g, [a], w21, w11, bt=1024)
        s11 = scatter(p11)
        gx = after(gx, s21)
        p20 = dw2_0(gx, a0, a1, h1, n)
        s20 = scatter(p20)
        gx = after(gx, p20, s11)
        p10, = bwd(x, gx, [a0, a1], w20, bt=1024)
        s10 = scatter(p10)
        d2 = jnp.stack([s20.reshape(D, -1).T, s21.reshape(D, -1).T])
        y, s10 = lax.optimization_barrier((fwd_y(after(x1, p10), h, w21), s10))
        return y.reshape(shape), jnp.stack([s10, s11]), d2

    return jax.shard_map(body, mesh=mesh, in_specs=(spec, spec, spec, spec),
                         out_specs=(spec, spec, spec), check_vma=False)
```

```python
import functools
import math

import jax
import jax.numpy as jnp
from jax import lax
from jax.experimental import pallas as pl
from jax.experimental.pallas import tpu as pltpu
from jax.sharding import PartitionSpec as P

AX = "fsdp"
D, FF = 768, 3072
G0 = 768
C0 = math.sqrt(2 / math.pi)
C1 = C0 * 0.044715
BF, F32 = jnp.bfloat16, jnp.float32


def gelu(a):
    t = jnp.tanh(a * (C0 + C1 * (a * a)))
    return a * (0.5 + 0.5 * t)


def gelu_grad(a):
    b = a * a
    s = 0.5 + 0.5 * jnp.tanh(a * (C0 + C1 * b))
    return s + ((a * s) * (1 - s)) * (2 * C0 + 6 * C1 * b)


def dot(a, b):
    return jnp.dot(a, b, preferred_element_type=F32)


def dot_nt(a, b):
    return lax.dot_general(a, b, (((1,), (1,)), ((), ())), preferred_element_type=F32)


def h_of(a):
    return gelu(a.astype(F32)).astype(BF)


def full(shape):
    return pl.BlockSpec(shape, lambda i: (0,) * len(shape), pipeline_mode=pl.Buffered(1))


def tok(bt, n):
    return pl.BlockSpec((bt, n), lambda i: (i, 0))


def sds(shape, dt=BF):
    return jax.ShapeDtypeStruct(shape, dt)


def call(name, body, t, bt, args, in_specs, out_specs, out_shape, scratch, dots):
    nbytes = sum(math.prod(v.shape) * v.dtype.itemsize for v in (*args, *out_shape))
    return pl.pallas_call(
        body, name=name, grid=(t // bt,), in_specs=in_specs, out_specs=out_specs, out_shape=out_shape,
        scratch_shapes=scratch,
        compiler_params=pltpu.CompilerParams(dimension_semantics=("arbitrary",), vmem_limit_bytes=67043328),
        cost_estimate=pl.CostEstimate(flops=int(dots * 2 * t * D * FF), bytes_accessed=nbytes, transcendentals=t * FF),
    )(*args)


def chunks(n, ch):
    return [slice(k, k + ch) for k in range(0, n, ch)]


def pieces(refs, ch):
    work, off = [], 0
    for r in refs:
        work += [(slice(off + s.start, off + s.stop), r, s) for s in chunks(r.shape[1], ch)]
        off += r.shape[1]
    return work


def fwd_a(x, w, bt=1024, ch=256):
    t, n = x.shape[0], w.shape[1]

    def body(x_ref, w_ref, a_ref):
        for s in chunks(n, ch):
            a_ref[:, s] = dot(x_ref[...], w_ref[:, s]).astype(BF)

    return call(f"fwd_a{n}", body, t, bt, (x, w), [tok(bt, D), full((D, n))], [tok(bt, n)], [sds((t, n))], [], n / FF)[0]


def fwd_y(x, a, w2, name, bt=1024, ch=256, rs=128):
    t, na = x.shape[0], len(a)

    def body(x_ref, w2_ref, *refs):
        y_ref, h_ref = refs[na:]

        def act(r):
            for c, ref, s in pieces(refs[:na], ch):
                h_ref[r, c] = h_of(ref[r, s])

        rows = chunks(bt, rs)
        act(rows[0])
        for k, r in enumerate(rows):
            if k + 1 < len(rows):
                act(rows[k + 1])
            y_ref[r, :] = (x_ref[r, :].astype(F32) + dot(h_ref[r, :], w2_ref[...])).astype(BF)

    return call(name, body, t, bt, (x, w2, *a), [tok(bt, D), full((FF, D)), *(tok(bt, v.shape[1]) for v in a)],
                [tok(bt, D)], [sds((t, D))], [pltpu.VMEM((bt, FF), BF)], 1)[0]


def zero_first(ref):
    @pl.when(pl.program_id(0) == 0)
    def _():
        ref[...] = jnp.zeros_like(ref)


def put_last(steps, acc, out_ref, sem):
    @pl.when(pl.program_id(0) == steps - 1)
    def _():
        n, _, w = out_ref.shape
        copies = [pltpu.make_async_copy(acc.at[:, k * w:(k + 1) * w], out_ref.at[k], sem.at[k]) for k in range(n)]
        for c in copies:
            c.start()
        for c in copies:
            c.wait()


def fwd_dw2(x, g, w1, n, bt=1024, ch=256):
    t = x.shape[0]

    def body(x_ref, g_ref, w1_ref, a_ref, out_ref, acc, gT, sem):
        zero_first(acc)
        ss = chunks(FF, ch)

        def first(s):
            a = dot(x_ref[...], w1_ref[:, s]).astype(BF)
            a_ref[:, s] = a
            return a

        a, prev = first(ss[0]), None
        gT[...] = g_ref[...].T
        for j, s in enumerate(ss):
            nxt = first(ss[j + 1]) if j + 1 < len(ss) else None
            h = h_of(a)
            if prev is not None:
                acc[:, ss[j - 1]] += dot(gT[...], prev)
            a, prev = nxt, h
        acc[:, ss[-1]] += dot(gT[...], prev)
        put_last(t // bt, acc, out_ref, sem)

    return call("fwd_dw2", body, t, bt, (x, g, w1), [tok(bt, D), tok(bt, D), full((D, FF))],
                [tok(bt, FF), pl.BlockSpec(memory_space=pl.ANY)],
                [sds((t, FF)), sds((n, D, FF // n), F32)],
                [pltpu.VMEM((D, FF), F32), pltpu.VMEM((D, bt), BF), pltpu.SemaphoreType.DMA((n,))], 2)


def dw2_0(g, a, n, bt=1024, ch=768):
    t, na = g.shape[0], len(a)

    def body(g_ref, *refs):
        out_ref, acc, gT, sem = refs[na:]
        zero_first(acc)
        gT[...] = g_ref[...].T
        for c, r, s in pieces(refs[:na], ch):
            acc[:, c] += dot(gT[...], h_of(r[:, s]))
        put_last(t // bt, acc, out_ref, sem)

    return call("dw2_0", body, t, bt, (g, *a), [tok(bt, D), *(tok(bt, v.shape[1]) for v in a)],
                [pl.BlockSpec(memory_space=pl.ANY)], [sds((n, D, FF // n), F32)],
                [pltpu.VMEM((D, FF), F32), pltpu.VMEM((D, bt), BF), pltpu.SemaphoreType.DMA((n,))], 1)[0]


def bwd(x, g, a, w2, w1=None, bt=512, ch=512, gq=1536):
    t = x.shape[0]
    na = len(a)

    def body(*refs):
        x_ref, g_ref, w2_ref, *rest = refs
        a_refs, rest = rest[:na], rest[na:]
        if w1 is None:
            dw_ref, xT = rest
        else:
            w1_ref, gx_ref, dw_ref, xT, gx_acc, da_ref = rest
        zero_first(dw_ref)
        work = pieces(a_refs, ch)

        def cot(k):
            return dot_nt(g_ref[...], w2_ref[work[k][0], :])

        def use(k, da):
            s = work[k][0]
            dw_ref[:, s] += dot(xT[...], da)
            if w1 is not None and s.stop % gq == 0:
                q = slice(s.stop - gq, s.stop)
                p = dot_nt(da_ref[:, q], w1_ref[:, q])
                if q.start:
                    p += gx_acc[...]
                if q.stop < FF:
                    gx_acc[...] = p
                else:
                    gx_ref[...] = (g_ref[...].astype(F32) + p).astype(BF)

        e, prev = cot(0), None
        xT[...] = x_ref[...].T
        for k, (_, r, s) in enumerate(work):
            nxt = cot(k + 1) if k + 1 < len(work) else None
            da = (gelu_grad(r[:, s].astype(F32)) * e).astype(BF)
            if w1 is not None:
                da_ref[:, work[k][0]] = da
            if prev is not None:
                use(k - 1, prev)
            e, prev = nxt, da
        use(len(work) - 1, prev)

    args, specs = [x, g, w2, *a], [tok(bt, D), tok(bt, D), full((FF, D)), *(tok(bt, v.shape[1]) for v in a)]
    outs, oshape = [full((D, FF))], [sds((D, FF), F32)]
    scratch = [pltpu.VMEM((D, bt), BF)]
    if w1 is not None:
        args, specs = [*args, w1], [*specs, full((D, FF))]
        outs, oshape = [tok(bt, D), *outs], [sds((t, D)), *oshape]
        scratch += [pltpu.VMEM((bt, D), F32), pltpu.VMEM((bt, FF), BF)]
    return call("bwd" if w1 is not None else "bwd0", body, t, bt, tuple(args), specs, outs, oshape, scratch,
                2 if w1 is None else 3)


def solution(mesh):
    spec = P(None, AX, None)
    n = mesh.shape[AX]

    def gather(w):
        return lax.all_gather(w, AX, axis=0, tiled=True)

    def scatter(v):
        return lax.psum_scatter(v, AX, scatter_dimension=0, tiled=True)

    def after(v, *done):
        return lax.optimization_barrier((v, *done))[0]

    def body(x, g, w1, w2):
        shape = x.shape
        x, g = x.reshape(-1, D), g.reshape(-1, D)
        w10a, w10b = gather(w1[0, :, :G0]), gather(w1[0, :, G0:])
        w20, w11, w21 = gather(w2[0]), gather(w1[1]), gather(w2[1])
        a0 = [fwd_a(x, w10a)]
        a0.append(fwd_a(after(x, a0[0]), w10b))
        x1 = fwd_y(x, a0, w20, "fwd_y0")
        a, p21 = fwd_dw2(x1, g, w11, n)
        s21 = scatter(p21)
        gx, p11 = bwd(x1, g, [a], w21, w11, bt=1024)
        s11 = scatter(p11)
        gx = after(gx, s21)
        p20 = dw2_0(gx, a0, n)
        s20 = scatter(p20)
        gx = after(gx, p20, s11)
        p10, = bwd(x, gx, a0, w20, bt=1024, ch=256)
        s10 = scatter(p10)
        y, s10 = lax.optimization_barrier((fwd_y(after(x1, p10, s20), [a], w21, "fwd_y1"), s10))
        d2 = jnp.stack([s20.reshape(D, -1).T, s21.reshape(D, -1).T])
        return y.reshape(shape), jnp.stack([s10, s11]), d2

    return jax.shard_map(body, mesh=mesh, in_specs=(spec, spec, spec, spec),
                         out_specs=(spec, spec, spec), check_vma=False)
```
